256 devices in a mesh: row: 16 (over z, x_lo), col: 16 (over x_hi, y, core).
Axes of the slice: x: 4 (x_hi: 2, x_lo: 2; x = x_hi * 2 + x_lo), y: 4, z: 8, core: 2. Of those that a mesh axis runs over, the one named last changes fastest.
Arguments:
- field: bfloat16 [128, 2048, 2048], P(None, 'row', 'col'), may hold values from -6 to 6
- solid_flags: int32 [128, 256, 128], P(None, 'row', 'col'), may hold values 0 or 1
- deriv_matrix: bfloat16 [2048, 2048], replicated, may hold values from -0.125 to 0.125
Outputs:
- filtered: bfloat16 [128, 2048, 2048], P('col', 'row')
- deriv_z: bfloat16 [128, 2048, 2048], P('col', 'row')
The draws below stay inside these ranges and needn't reach their ends.
Inputs may be any that keep to these rules, and one draw needn't show every extreme that they name: `solid_flags`: 1 marks a solid block, 0 a fluid one.
All inputs are finite; a program needn't handle non-finite values.
Results may differ from the reference program's by a relative error of at most 0.0058.
Values may be sent and summed in bfloat16 or wider, within the bound.
A program may use at most 64 MiB of HBM per device.

```python
import jax
import jax.numpy as jnp
from jax import lax

NZ = 2048
YBLK = 8
ZBLK = 16
NX = 128
NY = 2048


def plant(drawn, rng, least, high):
    spot = [jax.random.randint(jax.random.fold_in(rng, axis), (), 0, length) for axis, length in enumerate(drawn.shape)]
    longest = drawn.shape.index(max(drawn.shape))
    neighbour = spot[:longest] + [(spot[longest] + 1) % drawn.shape[longest]] + spot[longest + 1:]
    return drawn.at[tuple(spot)].set(least).at[tuple(neighbour)].set(high)


def level_of(stream_key, shape, split, smallest, top_value):
    gain = 1.0
    for axis_at, blocks in split:
        steps = jax.random.uniform(jax.random.fold_in(jax.random.fold_in(stream_key, 6), axis_at), (blocks,), jnp.float32, smallest / len(split), top_value / len(split))
        gain = gain * jnp.repeat(jnp.exp(steps), shape[axis_at] // blocks).reshape((-1,) + (1,) * (len(shape) - 1 - axis_at))
    return gain


def gaussian(stream_key, extent, scale, most, split=(), kind=jnp.bfloat16):
    values = jax.random.normal(stream_key, extent, jnp.float32) * scale
    if len(split) > 0:
        values = level_of(stream_key, extent, split, -0.22, 0.18) * values
    return jnp.clip(values, min=-most, max=most).astype(kind)


def setup_inputs(seed: int = 0) -> dict:
    keys = jax.random.split(jax.random.key(seed), 4)
    field = gaussian(keys[0], (NX, NY, NZ), 1.0, 6.0, ((1, 16), (2, 16)))
    solid_flags = plant((jax.random.randint(keys[1], (NX, NY // YBLK, NZ // ZBLK), 0, 4) < 1).astype(jnp.int32), jax.random.fold_in(keys[1], 1), 0, 1)
    deriv_matrix = gaussian(keys[2], (NZ, NZ), NZ ** -0.5, 0.125)
    return {"field": field, "solid_flags": solid_flags, "deriv_matrix": deriv_matrix}


filter_taps = ((-3, 1.0), (-2, -6.0), (-1, 15.0), (0, -20.0), (1, 15.0), (2, -6.0), (3, 1.0))


def smooth(values, axis):
    total = values
    for offset, tap in filter_taps:
        total = total + (tap / 64.0) * jnp.roll(values, -offset, axis)
    return total


def reference(field, solid_flags, deriv_matrix):
    def one_plane(inputs):
        plane, flags = inputs
        blocks = flags.astype(jnp.float32)
        nyb, nzb = blocks.shape
        solid = jnp.broadcast_to(blocks[:, None, :, None], (nyb, YBLK, nzb, ZBLK)).reshape(nyb * YBLK, nzb * ZBLK)
        masked = plane.astype(jnp.float32) * (1.0 - solid)
        yfilt = smooth(masked, 0).astype(jnp.bfloat16)
        filtered = smooth(yfilt.astype(jnp.float32), 1).astype(jnp.bfloat16)
        deriv = jnp.dot(filtered, deriv_matrix, preferred_element_type=jnp.float32).astype(jnp.bfloat16)
        return filtered, deriv

    filtered, deriv_z = lax.map(one_plane, (field, solid_flags))
    return filtered, deriv_z
```

```python
import functools

import jax
import jax.numpy as jnp
import numpy as np
from jax import lax
from jax.experimental import pallas as pl
from jax.experimental.pallas import tpu as pltpu
from jax.sharding import PartitionSpec as P

MESH = pl.DeviceIdType.MESH
YBLK = 8
ZBLK = 16
TAPS = {-3: 1.0, -2: -6.0, -1: 15.0, 0: 44.0, 1: 15.0, 2: -6.0, 3: 1.0}


def y_matrix(ny):
    out = np.zeros((ny, ny), np.float32)
    for r in range(ny):
        for o, tap in TAPS.items():
            if 0 <= r + o < ny:
                out[r, r + o] = tap / 64.0
    return out


def halo_matrix(lines):
    up = np.zeros((lines * 3, lines * 16), np.float32)
    down = np.zeros((lines * 3, lines * 16), np.float32)
    for l in range(lines):
        for j in range(3):
            for q in range(3):
                o = q - (j - 3)
                if o in TAPS:
                    up[l * 3 + j, l * 16 + q] = TAPS[o] / 64.0
                o = (q - 3) - j
                if o in TAPS:
                    down[l * 3 + j, l * 16 + 8 + 5 + q] = TAPS[o] / 64.0
    return np.concatenate([up, down], axis=0)


def spread_matrix(lines):
    out = np.zeros((lines * 16, lines * 6), np.float32)
    for l in range(lines):
        for j in range(3):
            out[l * 16 + 8 + 5 + j, l * 3 + j] = 1.0
            out[l * 16 + j, lines * 3 + l * 3 + j] = 1.0
    return out


def z_matrix(nz):
    out = np.zeros((4 * nz, 2 * nz), np.float32)
    for c in range(2 * nz):
        for o, tap in TAPS.items():
            out[nz + c + o, c] = tap / 64.0
    return out


def expand_matrix(nzb):
    return np.repeat(np.eye(nzb, dtype=np.float32), ZBLK, axis=1)


def exchange_kernel(
    nrow, ncol, order,
    field, flags_in, dmat, fy_in, ch_in, sp_in, bz_in, ex_in,
    filt, der, tail, dv,
    fbuf, etop, ebot, mask, ybuf, recv, hup, hdown, hfrom_next, hfrom_prev, edges, fy, ch, sp, bz, ex, flags,
    in_sem, fsem, send_sem, recv_sem, hsend_sem, hrecv_sem,
):
    row, col = lax.axis_index("row"), lax.axis_index("col")
    above, below = lax.rem(row + nrow - 1, nrow), lax.rem(row + 1, nrow)
    lines, ny, nz = fbuf.shape[0], fbuf.shape[2], fbuf.shape[3]
    nyb = flags.shape[0]

    flag_loads = [
        pltpu.make_async_copy(flags_in, flags, in_sem.at[7]),
        pltpu.make_async_copy(ex_in, ex, in_sem.at[8]),
    ]
    for copy in flag_loads:
        copy.start()
    loads = [
        pltpu.make_async_copy(field.at[:, :, pl.ds(0, 8), :], etop, in_sem.at[0]),
        pltpu.make_async_copy(field.at[:, :, pl.ds(ny - 8, 8), :], ebot, in_sem.at[1]),
        pltpu.make_async_copy(ch_in, ch, in_sem.at[2]),
        pltpu.make_async_copy(fy_in, fy, in_sem.at[3]),
    ]
    for copy in loads:
        copy.start()
    field_loads = [pltpu.make_async_copy(field.at[:, k], fbuf.at[k], fsem.at[k]) for k in range(lines)]
    for copy in field_loads:
        copy.start()
    late = [
        pltpu.make_async_copy(sp_in, sp, in_sem.at[4]),
        pltpu.make_async_copy(bz_in, bz, in_sem.at[5]),
        pltpu.make_async_copy(dmat, dv, in_sem.at[6]),
    ]
    for copy in late:
        copy.start()

    barrier = pltpu.get_barrier_semaphore()
    for s in range(1, ncol):
        pl.semaphore_signal(
            barrier, inc=1, device_id={"row": row, "col": lax.rem(col + s, ncol)}, device_id_type=MESH
        )
    for r in (above, below):
        for s in range(ncol):
            pl.semaphore_signal(
                barrier, inc=1, device_id={"row": r, "col": lax.rem(col + s, ncol)}, device_id_type=MESH
            )

    for copy in flag_loads:
        copy.wait()
    for b in range(nyb):
        solid = lax.dot_general(
            flags[b].astype(jnp.float32), ex[...], (((0,), (0,)), ((), ())), preferred_element_type=jnp.float32
        )
        mask[b] = 1.0 - solid

    def mask_rows(b, x):
        return jnp.broadcast_to(mask[b, pl.ds(x, 1), :], (YBLK, nz))

    for copy in loads:
        copy.wait()

    @pl.loop(0, ncol)
    def _(d):
        parts = []
        for l in range(lines):
            x = d * lines + l
            parts.append(etop[d, l].astype(jnp.float32) * mask_rows(0, x))
            parts.append(ebot[d, l].astype(jnp.float32) * mask_rows(nyb - 1, x))
        edge = jnp.concatenate(parts, axis=0).astype(jnp.bfloat16)
        halo = jnp.dot(ch[...], edge, preferred_element_type=jnp.float32).astype(jnp.bfloat16)
        hup[d] = halo[: 3 * lines]
        hdown[d] = halo[3 * lines :]

    pl.semaphore_wait(barrier, ncol - 1 + 2 * ncol)

    def halo_copy(src, dst, r, d, way):
        return pltpu.make_async_remote_copy(
            src_ref=src.at[d],
            dst_ref=dst.at[col],
            send_sem=hsend_sem.at[way],
            recv_sem=hrecv_sem.at[way],
            device_id={"row": r, "col": d},
            device_id_type=MESH,
        )

    @pl.loop(0, ncol)
    def _(s):
        d = lax.rem(col + s, ncol)
        halo_copy(hup, hfrom_next, above, d, 0).start()
        halo_copy(hdown, hfrom_prev, below, d, 1).start()

    def line_copy(k, d):
        return pltpu.make_async_remote_copy(
            src_ref=ybuf.at[k, d],
            dst_ref=recv.at[k, col],
            send_sem=send_sem.at[k],
            recv_sem=recv_sem.at[k],
            device_id={"row": row, "col": d},
            device_id_type=MESH,
        )

    @pl.loop(0, lines)
    def _(k):
        pltpu.make_async_copy(field.at[:, k], fbuf.at[k], fsem.at[k]).wait()

        @pl.loop(0, ncol // 2)
        def _(p):
            parts = []
            for h in range(2):
                d = 2 * p + h
                x = d * lines + k
                keep = jnp.concatenate([mask_rows(b, x) for b in range(nyb)], axis=0)
                parts.append((fbuf[k, d].astype(jnp.float32) * keep).astype(jnp.bfloat16))
            out = jnp.dot(fy[...], jnp.concatenate(parts, axis=1), preferred_element_type=jnp.float32)
            ybuf[k, 2 * p] = out[:, :nz].astype(jnp.bfloat16)
            ybuf[k, 2 * p + 1] = out[:, nz:].astype(jnp.bfloat16)

        for flip in order:
            line_copy(k, lax.rem(col + flip, ncol)).start()
        recv[k, col] = ybuf[k, col]

    for copy in late:
        copy.wait()

    def z_filter(block, j):
        near = [block((2 * j + o) % ncol) for o in (-1, 0, 1, 2)]
        out = jnp.dot(jnp.concatenate(near, axis=1), bz[...], preferred_element_type=jnp.float32)
        return out.astype(jnp.bfloat16)

    inner = pl.ds(8, ny - 16)

    def smooth_line(k):
        arrived = recv.at[k, pl.ds(0, ncol - 1)]
        pltpu.make_async_copy(arrived, arrived, recv_sem.at[k]).wait()
        for j in range(ncol // 2):
            filt[k, inner, pl.ds(2 * j * nz, 2 * nz)] = z_filter(lambda c: recv[k, c, inner, :], j)

    @pl.loop(0, lines - 1)
    def _(k):
        smooth_line(k)

        @pl.loop(0, ncol // 2)
        def _(n):
            at = pl.ds(pl.multiple_of(n * (2 * nz), 2 * nz), 2 * nz)
            out = jnp.dot(filt[k, inner, :], dv[:, at], preferred_element_type=jnp.float32)
            der[k, inner, at] = out.astype(jnp.bfloat16)

    last = lines - 1
    smooth_line(last)
    tail[pl.ds(0, ny - 16), :] = filt[last, inner, :]
    for way, ref in ((0, hfrom_next), (1, hfrom_prev)):
        pltpu.make_async_copy(ref, ref, hrecv_sem.at[way]).wait()

    @pl.loop(0, ncol)
    def _(c):
        halo = jnp.concatenate([hfrom_next[c].astype(jnp.float32), hfrom_prev[c].astype(jnp.float32)], axis=0)
        spread = jnp.dot(sp[...], halo.astype(jnp.bfloat16), preferred_element_type=jnp.float32)
        own = []
        for l in range(lines):
            own.append(recv[l, c, pl.ds(0, 8), :].astype(jnp.float32))
            own.append(recv[l, c, pl.ds(ny - 8, 8), :].astype(jnp.float32))
        edges[c] = (jnp.concatenate(own, axis=0) + spread).astype(jnp.bfloat16)

    for j in range(ncol // 2):
        at = pl.ds(2 * j * nz, 2 * nz)
        out = z_filter(lambda c: edges[c], j)
        tail[pl.ds(ny - 16, 16 * lines), at] = out
        for l in range(lines):
            filt[l, pl.ds(0, 8), at] = out[16 * l : 16 * l + 8]
            filt[l, pl.ds(ny - 8, 8), at] = out[16 * l + 8 : 16 * l + 16]

    for k in range(lines):
        sent = ybuf.at[k, pl.ds(0, ncol - 1)]
        pltpu.make_async_copy(sent, sent, send_sem.at[k]).wait()
    for way, ref in ((0, hup), (1, hdown)):
        pltpu.make_async_copy(ref, ref, hsend_sem.at[way]).wait()


def finish_kernel(filt, der, tail, dv, filt_out, der_out, dtail, sem, tail_sem):
    lines, ny, full = filt.shape
    inner = pl.ds(8, ny - 16)
    done = pl.ds(0, lines - 1)
    copies = [
        pltpu.make_async_copy(filt, filt_out, sem.at[0]),
        pltpu.make_async_copy(der.at[done, inner, :], der_out.at[done, inner, :], sem.at[1]),
    ]
    for copy in copies:
        copy.start()
    parts = 2
    width = full // parts
    for h in range(parts):

        @pl.loop(h * (width // 256), (h + 1) * (width // 256))
        def _(n):
            at = pl.ds(pl.multiple_of(n * 256, 256), 256)
            dtail[:, at] = jnp.dot(tail[...], dv[:, at], preferred_element_type=jnp.float32).astype(jnp.bfloat16)

        at = pl.ds(h * width, width)
        rows = ny - 16
        copies.append(
            pltpu.make_async_copy(
                dtail.at[pl.ds(0, rows), at], der_out.at[lines - 1, inner, at], tail_sem.at[h, 2 * lines]
            )
        )
        copies[-1].start()
        for l in range(lines):
            for e, lo in enumerate((0, ny - 8)):
                copies.append(
                    pltpu.make_async_copy(
                        dtail.at[pl.ds(rows + 16 * l + 8 * e, 8), at],
                        der_out.at[l, pl.ds(lo, 8), at],
                        tail_sem.at[h, 2 * l + e],
                    )
                )
                copies[-1].start()
    for copy in copies:
        copy.wait()


def shards(nrow, ncol, field, solid_flags, deriv_matrix):
    nx, ny, nz = field.shape
    nyb, nzb = solid_flags.shape[1:]
    lines = nx // ncol
    full = nz * ncol
    bf16, f32 = jnp.bfloat16, jnp.float32
    order = [s for s in range(1, ncol)]
    out = (lines, ny, full)
    any_spec = pl.BlockSpec(memory_space=pl.ANY)
    vmem = pl.BlockSpec(memory_space=pltpu.VMEM)
    consts = [
        jnp.asarray(y_matrix(ny), bf16),
        jnp.asarray(halo_matrix(lines), bf16),
        jnp.asarray(spread_matrix(lines), bf16),
        jnp.asarray(z_matrix(nz), bf16),
        jnp.asarray(expand_matrix(nzb), f32),
    ]
    tail = ny - 16 + 16 * lines
    held = pl.pallas_call(
        functools.partial(exchange_kernel, nrow, ncol, order),
        name="exchange",
        out_shape=[pltpu.VMEM(shape, bf16) for shape in (out, out, (tail, full), (full, full))],
        in_specs=[any_spec, any_spec, any_spec, any_spec, any_spec, any_spec, any_spec, any_spec],
        out_specs=[vmem] * 4,
        scratch_shapes=[
            pltpu.VMEM((lines, ncol, ny, nz), bf16),
            pltpu.VMEM((ncol, lines, 8, nz), bf16),
            pltpu.VMEM((ncol, lines, 8, nz), bf16),
            pltpu.VMEM((nyb, nx, nz), f32),
            pltpu.VMEM((lines, ncol, ny, nz), bf16),
            pltpu.VMEM((lines, ncol, ny, nz), bf16),
            pltpu.VMEM((ncol, 3 * lines, nz), bf16),
            pltpu.VMEM((ncol, 3 * lines, nz), bf16),
            pltpu.VMEM((ncol, 3 * lines, nz), bf16),
            pltpu.VMEM((ncol, 3 * lines, nz), bf16),
            pltpu.VMEM((ncol, 16 * lines, nz), bf16),
            *[pltpu.VMEM(c.shape, c.dtype) for c in consts],
            pltpu.VMEM((nyb, nzb, nx), jnp.int32),
            pltpu.SemaphoreType.DMA((9,)),
            pltpu.SemaphoreType.DMA((lines,)),
            pltpu.SemaphoreType.DMA((lines,)),
            pltpu.SemaphoreType.DMA((lines,)),
            pltpu.SemaphoreType.DMA((2,)),
            pltpu.SemaphoreType.DMA((2,)),
        ],
        compiler_params=pltpu.CompilerParams(
            collective_id=0, has_side_effects=True, vmem_limit_bytes=45 * 1024 * 1024
        ),
    )(
        field.reshape(ncol, lines, ny, nz),
        jnp.transpose(solid_flags, (1, 2, 0)),
        deriv_matrix,
        *consts,
    )
    return pl.pallas_call(
        finish_kernel,
        name="finish",
        out_shape=[jax.ShapeDtypeStruct(out, bf16)] * 2,
        in_specs=[vmem] * 4,
        out_specs=[any_spec, any_spec],
        scratch_shapes=[
            pltpu.VMEM((tail, full), bf16),
            pltpu.SemaphoreType.DMA((2,)),
            pltpu.SemaphoreType.DMA((2, 2 * lines + 1)),
        ],
        compiler_params=pltpu.CompilerParams(vmem_limit_bytes=8 * 1024 * 1024),
    )(*held)


def solution(mesh):
    in_specs = (P(None, "row", "col"), P(None, "row", "col"), P())
    out_specs = (P("col", "row", None), P("col", "row", None))
    body = functools.partial(shards, mesh.shape["row"], mesh.shape["col"])
    return jax.shard_map(body, mesh=mesh, in_specs=in_specs, out_specs=out_specs, check_vma=False)
```

```python
import functools

import jax
import jax.numpy as jnp
import numpy as np
from jax import lax
from jax.experimental import pallas as pl
from jax.experimental.pallas import tpu as pltpu
from jax.sharding import PartitionSpec as P

MESH = pl.DeviceIdType.MESH
YBLK = 8
ZBLK = 16
TAPS = {-3: 1.0, -2: -6.0, -1: 15.0, 0: 44.0, 1: 15.0, 2: -6.0, 3: 1.0}


def y_matrix(ny):
    out = np.zeros((ny, ny), np.float32)
    for r in range(ny):
        for o, tap in TAPS.items():
            if 0 <= r + o < ny:
                out[r, r + o] = tap / 64.0
    return out


def halo_matrix(lines):
    up = np.zeros((lines * 3, lines * 16), np.float32)
    down = np.zeros((lines * 3, lines * 16), np.float32)
    for l in range(lines):
        for j in range(3):
            for q in range(3):
                o = q - (j - 3)
                if o in TAPS:
                    up[l * 3 + j, l * 16 + q] = TAPS[o] / 64.0
                o = (q - 3) - j
                if o in TAPS:
                    down[l * 3 + j, l * 16 + 8 + 5 + q] = TAPS[o] / 64.0
    return np.concatenate([up, down], axis=0)


def spread_matrix(lines):
    out = np.zeros((lines * 16, lines * 6), np.float32)
    for l in range(lines):
        for j in range(3):
            out[l * 16 + 8 + 5 + j, l * 3 + j] = 1.0
            out[l * 16 + j, lines * 3 + l * 3 + j] = 1.0
    return out


def z_matrix(nz):
    out = np.zeros((4 * nz, 2 * nz), np.float32)
    for c in range(2 * nz):
        for o, tap in TAPS.items():
            out[nz + c + o, c] = tap / 64.0
    return out


def expand_matrix(nyb, nzb):
    return np.kron(np.eye(nyb, dtype=np.float32), np.repeat(np.eye(nzb, dtype=np.float32), ZBLK, axis=1))


def exchange_kernel(
    nrow, ncol, order,
    field, flags_in, dmat, fy_in, ch_in, sp_in, bz_in, ex_in,
    filt, der, tail, dv,
    fbuf, etop, ebot, mask, mbuf, ybuf, recv, hup, hdown, hfrom_next, hfrom_prev, spread, edges,
    fy, ch, sp, bz, ex, flags,
    in_sem, fsem, send_sem, recv_sem, hsend_sem, hrecv_sem,
):
    row, col = lax.axis_index("row"), lax.axis_index("col")
    above, below = lax.rem(row + nrow - 1, nrow), lax.rem(row + 1, nrow)
    lines, ny, nz = fbuf.shape[0], fbuf.shape[2], fbuf.shape[3]
    nyb = ny // YBLK
    bf16, f32 = jnp.bfloat16, jnp.float32

    flag_loads = [
        pltpu.make_async_copy(flags_in, flags, in_sem.at[7]),
        pltpu.make_async_copy(ex_in, ex, in_sem.at[8]),
        pltpu.make_async_copy(fy_in, fy, in_sem.at[3]),
    ]
    field_loads = [pltpu.make_async_copy(field.at[:, k], fbuf.at[k], fsem.at[k]) for k in range(lines)]
    edge_loads = [
        pltpu.make_async_copy(field.at[:, :, pl.ds(0, 8), :], etop, in_sem.at[0]),
        pltpu.make_async_copy(field.at[:, :, pl.ds(ny - 8, 8), :], ebot, in_sem.at[1]),
        pltpu.make_async_copy(ch_in, ch, in_sem.at[2]),
    ]
    late = [
        pltpu.make_async_copy(sp_in, sp, in_sem.at[4]),
        pltpu.make_async_copy(bz_in, bz, in_sem.at[5]),
        pltpu.make_async_copy(dmat, dv, in_sem.at[6]),
    ]
    for copy in [*flag_loads, field_loads[0], *edge_loads, *field_loads[1:], *late]:
        copy.start()

    barrier = pltpu.get_barrier_semaphore()
    for s in range(1, ncol):
        pl.semaphore_signal(
            barrier, inc=1, device_id={"row": row, "col": lax.rem(col + s, ncol)}, device_id_type=MESH
        )
    for r in (above, below):
        for s in range(ncol):
            pl.semaphore_signal(
                barrier, inc=1, device_id={"row": r, "col": lax.rem(col + s, ncol)}, device_id_type=MESH
            )

    for copy in flag_loads:
        copy.wait()
    per_line = flags[...].astype(f32).T.astype(bf16)
    for n in range(nyb // 4):
        solid = jnp.dot(per_line, ex[:, pl.ds(n * 4 * nz, 4 * nz)], preferred_element_type=f32)
        for b in range(4):
            mask[4 * n + b] = 1.0 - solid[:, b * nz : (b + 1) * nz]

    def mask_rows(b, x):
        return jnp.broadcast_to(mask[b, pl.ds(x, 1), :], (YBLK, nz))

    def filter_lines(k):
        for d in range(ncol):
            x = d * lines + k
            keep = jnp.concatenate([mask_rows(b, x) for b in range(nyb)], axis=0)
            mbuf[:, pl.ds(d * nz, nz)] = (fbuf[k, d].astype(f32) * keep).astype(bf16)
        for n in range(ncol // 4):
            out = jnp.dot(fy[...], mbuf[:, pl.ds(n * 4 * nz, 4 * nz)], preferred_element_type=f32)
            for i in range(4):
                ybuf[k, 4 * n + i] = out[:, i * nz : (i + 1) * nz].astype(bf16)

    def send_lines(k):
        for a, b, c in order:
            d = (lax.rem(col // 8 + a, 2) * 4 + lax.rem(col // 2 + b, 4)) * 2 + lax.rem(col + c, 2)
            pltpu.make_async_remote_copy(
                src_ref=ybuf.at[k, d],
                dst_ref=recv.at[k, col],
                send_sem=send_sem.at[k],
                recv_sem=recv_sem.at[k],
                device_id={"row": row, "col": d},
                device_id_type=MESH,
            ).start()
        recv[k, col] = ybuf[k, col]

    def halo_copy(src, dst, r, d, way):
        return pltpu.make_async_remote_copy(
            src_ref=src.at[d],
            dst_ref=dst.at[col],
            send_sem=hsend_sem.at[way],
            recv_sem=hrecv_sem.at[way],
            device_id={"row": r, "col": d},
            device_id_type=MESH,
        )

    field_loads[0].wait()
    filter_lines(0)
    pl.semaphore_wait(barrier, ncol - 1 + 2 * ncol)
    send_lines(0)

    for copy in edge_loads:
        copy.wait()
    for d in range(ncol):
        parts = []
        for l in range(lines):
            x = d * lines + l
            parts.append(etop[d, l].astype(f32) * mask_rows(0, x))
            parts.append(ebot[d, l].astype(f32) * mask_rows(nyb - 1, x))
        mbuf[:, pl.ds(d * nz, nz)] = jnp.concatenate(parts, axis=0).astype(bf16)
    for n in range(ncol // 4):
        halo = jnp.dot(ch[...], mbuf[:, pl.ds(n * 4 * nz, 4 * nz)], preferred_element_type=f32).astype(bf16)
        for i in range(4):
            hup[4 * n + i] = halo[: 3 * lines, i * nz : (i + 1) * nz]
            hdown[4 * n + i] = halo[3 * lines :, i * nz : (i + 1) * nz]

    @pl.loop(0, ncol)
    def _(s):
        d = lax.rem(col + s, ncol)
        halo_copy(hup, hfrom_next, above, d, 0).start()
        halo_copy(hdown, hfrom_prev, below, d, 1).start()

    @pl.loop(1, lines)
    def _(k):
        pltpu.make_async_copy(field.at[:, k], fbuf.at[k], fsem.at[k]).wait()
        filter_lines(k)
        send_lines(k)

    for copy in late:
        copy.wait()

    def z_filter(block, j):
        near = [block((2 * j + o) % ncol) for o in (-1, 0, 1, 2)]
        out = jnp.dot(jnp.concatenate(near, axis=1), bz[...], preferred_element_type=f32)
        return out.astype(bf16)

    def arrive(k):
        arrived = recv.at[k, pl.ds(0, ncol - 1)]
        pltpu.make_async_copy(arrived, arrived, recv_sem.at[k]).wait()

    inner = pl.ds(8, ny - 16)
    last = lines - 1

    @pl.loop(0, last)
    def _(k):
        arrive(k)
        for j in range(ncol // 2):
            filt[k, inner, pl.ds(2 * j * nz, 2 * nz)] = z_filter(lambda c: recv[k, c, inner, :], j)

        @pl.loop(0, ncol // 2)
        def _(n):
            at = pl.ds(pl.multiple_of(n * (2 * nz), 2 * nz), 2 * nz)
            der[k, inner, at] = jnp.dot(filt[k, inner, :], dv[:, at], preferred_element_type=f32).astype(bf16)

    for way, ref in ((0, hfrom_next), (1, hfrom_prev)):
        pltpu.make_async_copy(ref, ref, hrecv_sem.at[way]).wait()
    for n in range(ncol // 4):
        halo = [
            jnp.concatenate([hfrom_next[c].astype(f32), hfrom_prev[c].astype(f32)], axis=0).astype(bf16)
            for c in range(4 * n, 4 * n + 4)
        ]
        out = jnp.dot(sp[...], jnp.concatenate(halo, axis=1), preferred_element_type=f32)
        for i in range(4):
            spread[4 * n + i] = out[:, i * nz : (i + 1) * nz]
    for c in range(ncol):
        own = []
        for l in range(last):
            own.append(recv[l, c, pl.ds(0, 8), :].astype(f32))
            own.append(recv[l, c, pl.ds(ny - 8, 8), :].astype(f32))
        edges[c] = (jnp.concatenate(own, axis=0) + spread[c, pl.ds(0, 16 * last), :]).astype(bf16)
    for j in range(ncol // 2):
        at = pl.ds(2 * j * nz, 2 * nz)
        out = z_filter(lambda c: edges[c], j)
        tail[pl.ds(ny, 16 * last), at] = out
        for l in range(last):
            filt[l, pl.ds(0, 8), at] = out[16 * l : 16 * l + 8]
            filt[l, pl.ds(ny - 8, 8), at] = out[16 * l + 8 : 16 * l + 16]

    arrive(last)
    for c in range(ncol):
        for lo, at in ((0, 0), (ny - 8, 8)):
            rows = pl.ds(lo, 8)
            recv[last, c, rows, :] = (
                recv[last, c, rows, :].astype(f32) + spread[c, pl.ds(16 * last + at, 8), :]
            ).astype(bf16)
    for j in range(ncol // 2):
        at = pl.ds(2 * j * nz, 2 * nz)
        out = z_filter(lambda c: recv[last, c], j)
        tail[pl.ds(0, ny), at] = out
        filt[last, :, at] = out

    for k in range(lines):
        sent = ybuf.at[k, pl.ds(0, ncol - 1)]
        pltpu.make_async_copy(sent, sent, send_sem.at[k]).wait()
    for way, ref in ((0, hup), (1, hdown)):
        pltpu.make_async_copy(ref, ref, hsend_sem.at[way]).wait()


def finish_kernel(filt, der, tail, dv, filt_out, der_out, dtail, sem, tail_sem):
    lines, ny, full = filt.shape
    inner = pl.ds(8, ny - 16)
    done = pl.ds(0, lines - 1)
    copies = [
        pltpu.make_async_copy(filt, filt_out, sem.at[0]),
        pltpu.make_async_copy(der.at[done, inner, :], der_out.at[done, inner, :], sem.at[1]),
    ]
    for copy in copies:
        copy.start()
    parts = 2
    width = full // parts
    for h in range(parts):
        at = pl.ds(h * width, width)
        dtail[:, at] = jnp.dot(tail[...], dv[:, at], preferred_element_type=jnp.float32).astype(jnp.bfloat16)
        copies.append(
            pltpu.make_async_copy(
                dtail.at[pl.ds(0, ny), at], der_out.at[lines - 1, :, at], tail_sem.at[h, 2 * lines - 2]
            )
        )
        copies[-1].start()
        for l in range(lines - 1):
            for e, lo in enumerate((0, ny - 8)):
                copies.append(
                    pltpu.make_async_copy(
                        dtail.at[pl.ds(ny + 16 * l + 8 * e, 8), at],
                        der_out.at[l, pl.ds(lo, 8), at],
                        tail_sem.at[h, 2 * l + e],
                    )
                )
                copies[-1].start()
    for copy in copies:
        copy.wait()


def shards(nrow, ncol, field, solid_flags, deriv_matrix):
    nx, ny, nz = field.shape
    nyb, nzb = solid_flags.shape[1:]
    lines = nx // ncol
    full = nz * ncol
    bf16, f32 = jnp.bfloat16, jnp.float32
    along_x = [(1, b, c) for b in (2, 1, 3, 0) for c in (0, 1)]
    along_y = [(0, b, c) for b in (2, 1, 3) for c in (0, 1)] + [(0, 0, 1)]
    order = [step for pair in zip(along_x, along_y) for step in pair] + along_x[len(along_y) :]
    out = (lines, ny, full)
    any_spec = pl.BlockSpec(memory_space=pl.ANY)
    vmem = pl.BlockSpec(memory_space=pltpu.VMEM)
    consts = [
        jnp.asarray(y_matrix(ny), bf16),
        jnp.asarray(halo_matrix(lines), bf16),
        jnp.asarray(spread_matrix(lines), bf16),
        jnp.asarray(z_matrix(nz), bf16),
        jnp.asarray(expand_matrix(nyb, nzb), bf16),
    ]
    tail = ny + 16 * (lines - 1)
    held = pl.pallas_call(
        functools.partial(exchange_kernel, nrow, ncol, order),
        name="exchange",
        out_shape=[pltpu.VMEM(shape, bf16) for shape in (out, out, (tail, full), (full, full))],
        in_specs=[any_spec, any_spec, any_spec, any_spec, any_spec, any_spec, any_spec, any_spec],
        out_specs=[vmem] * 4,
        scratch_shapes=[
            pltpu.VMEM((lines, ncol, ny, nz), bf16),
            pltpu.VMEM((ncol, lines, 8, nz), bf16),
            pltpu.VMEM((ncol, lines, 8, nz), bf16),
            pltpu.VMEM((nyb, nx, nz), f32),
            pltpu.VMEM((ny, full), bf16),
            pltpu.VMEM((lines, ncol, ny, nz), bf16),
            pltpu.VMEM((lines, ncol, ny, nz), bf16),
            pltpu.VMEM((ncol, 3 * lines, nz), bf16),
            pltpu.VMEM((ncol, 3 * lines, nz), bf16),
            pltpu.VMEM((ncol, 3 * lines, nz), bf16),
            pltpu.VMEM((ncol, 3 * lines, nz), bf16),
            pltpu.VMEM((ncol, 16 * lines, nz), f32),
            pltpu.VMEM((ncol, 16 * (lines - 1), nz), bf16),
            *[pltpu.VMEM(c.shape, c.dtype) for c in consts],
            pltpu.VMEM((nyb * nzb, nx), jnp.int32),
            pltpu.SemaphoreType.DMA((9,)),
            pltpu.SemaphoreType.DMA((lines,)),
            pltpu.SemaphoreType.DMA((lines,)),
            pltpu.SemaphoreType.DMA((lines,)),
            pltpu.SemaphoreType.DMA((2,)),
            pltpu.SemaphoreType.DMA((2,)),
        ],
        compiler_params=pltpu.CompilerParams(
            collective_id=0, has_side_effects=True, vmem_limit_bytes=45 * 1024 * 1024
        ),
    )(
        field.reshape(ncol, lines, ny, nz),
        jnp.transpose(solid_flags, (1, 2, 0)).reshape(nyb * nzb, nx),
        deriv_matrix,
        *consts,
    )
    return pl.pallas_call(
        finish_kernel,
        name="finish",
        out_shape=[jax.ShapeDtypeStruct(out, bf16)] * 2,
        in_specs=[vmem] * 4,
        out_specs=[any_spec, any_spec],
        scratch_shapes=[
            pltpu.VMEM((tail, full), bf16),
            pltpu.SemaphoreType.DMA((2,)),
            pltpu.SemaphoreType.DMA((2, 2 * lines - 1)),
        ],
        compiler_params=pltpu.CompilerParams(vmem_limit_bytes=8 * 1024 * 1024),
    )(*held)


def solution(mesh):
    in_specs = (P(None, "row", "col"), P(None, "row", "col"), P())
    out_specs = (P("col", "row", None), P("col", "row", None))
    body = functools.partial(shards, mesh.shape["row"], mesh.shape["col"])
    return jax.shard_map(body, mesh=mesh, in_specs=in_specs, out_specs=out_specs, check_vma=False)
```

```python
import functools

import jax
import jax.numpy as jnp
import numpy as np
from jax import lax
from jax.experimental import pallas as pl
from jax.experimental.pallas import tpu as pltpu
from jax.sharding import PartitionSpec as P

MESH = pl.DeviceIdType.MESH
GATE = 1
EARLY = 5
YBLK = 8
ZBLK = 16
TAPS = {-3: 1.0, -2: -6.0, -1: 15.0, 0: 44.0, 1: 15.0, 2: -6.0, 3: 1.0}


def y_matrix(ny):
    out = np.zeros((ny, ny), np.float32)
    for r in range(ny):
        for o, tap in TAPS.items():
            if 0 <= r + o < ny:
                out[r, r + o] = tap / 64.0
    return out


def halo_matrix(lines):
    up = np.zeros((lines * 3, lines * 16), np.float32)
    down = np.zeros((lines * 3, lines * 16), np.float32)
    for l in range(lines):
        for j in range(3):
            for q in range(3):
                o = q - (j - 3)
                if o in TAPS:
                    up[l * 3 + j, l * 16 + q] = TAPS[o] / 64.0
                o = (q - 3) - j
                if o in TAPS:
                    down[l * 3 + j, l * 16 + 8 + 5 + q] = TAPS[o] / 64.0
    return np.concatenate([up, down], axis=0)


def spread_matrix(lines):
    out = np.zeros((lines * 16, lines * 6), np.float32)
    for l in range(lines):
        for j in range(3):
            out[l * 16 + 8 + 5 + j, l * 3 + j] = 1.0
            out[l * 16 + j, lines * 3 + l * 3 + j] = 1.0
    return out


def z_matrix(nz):
    out = np.zeros((4 * nz, 2 * nz), np.float32)
    for c in range(2 * nz):
        for o, tap in TAPS.items():
            out[nz + c + o, c] = tap / 64.0
    return out


def expand_matrix(nyb, nzb):
    return np.kron(np.eye(nyb, dtype=np.float32), np.repeat(np.eye(nzb, dtype=np.float32), ZBLK, axis=1))


def exchange_kernel(
    nrow, ncol, order,
    field, flags_in, dmat, fy_in, ch_in, sp_in, bz_in, ex_in,
    filt, der, tail, dv,
    fbuf, etop, ebot, mask, mbuf, ybuf, recv, hup, hdown, hfrom_next, hfrom_prev, spread, edges,
    fy, ch, sp, bz, ex, flags,
    in_sem, fsem, send_sem, recv_sem, hsend_sem, hrecv_sem, joined, rows_in,
):
    row, col = lax.axis_index("row"), lax.axis_index("col")
    above, below = lax.rem(row + nrow - 1, nrow), lax.rem(row + 1, nrow)
    lines, ny, nz = fbuf.shape[0], fbuf.shape[2], fbuf.shape[3]
    nyb = ny // YBLK
    bf16, f32 = jnp.bfloat16, jnp.float32

    flag_loads = [
        pltpu.make_async_copy(flags_in, flags, in_sem.at[7]),
        pltpu.make_async_copy(ex_in, ex, in_sem.at[8]),
        pltpu.make_async_copy(fy_in, fy, in_sem.at[3]),
    ]
    field_loads = [pltpu.make_async_copy(field.at[:, k], fbuf.at[k], fsem.at[k]) for k in range(lines)]
    edge_loads = [
        pltpu.make_async_copy(field.at[:, :, pl.ds(0, 8), :], etop, in_sem.at[0]),
        pltpu.make_async_copy(field.at[:, :, pl.ds(ny - 8, 8), :], ebot, in_sem.at[1]),
        pltpu.make_async_copy(ch_in, ch, in_sem.at[2]),
    ]
    late = [
        pltpu.make_async_copy(sp_in, sp, in_sem.at[4]),
        pltpu.make_async_copy(bz_in, bz, in_sem.at[5]),
        pltpu.make_async_copy(dmat, dv, in_sem.at[6]),
    ]
    for copy in [*flag_loads, field_loads[0], *edge_loads, *field_loads[1:], *late]:
        copy.start()

    barrier = pltpu.get_barrier_semaphore()
    for s in range(1, ncol):
        d = lax.rem(col + s, ncol)

        @pl.when(d != GATE)
        def _():
            pl.semaphore_signal(barrier, inc=1, device_id={"row": row, "col": d}, device_id_type=MESH)

    for copy in flag_loads:
        copy.wait()
    per_line = flags[...].astype(f32).T.astype(bf16)
    for n in range(nyb // 4):
        solid = jnp.dot(per_line, ex[:, pl.ds(n * 4 * nz, 4 * nz)], preferred_element_type=f32)
        for b in range(4):
            mask[4 * n + b] = 1.0 - solid[:, b * nz : (b + 1) * nz]

    def mask_rows(b, x):
        return jnp.broadcast_to(mask[b, pl.ds(x, 1), :], (YBLK, nz))

    def filter_lines(k):
        for d in range(ncol):
            x = d * lines + k
            keep = jnp.concatenate([mask_rows(b, x) for b in range(nyb)], axis=0)
            mbuf[:, pl.ds(d * nz, nz)] = (fbuf[k, d].astype(f32) * keep).astype(bf16)
        for n in range(ncol // 4):
            out = jnp.dot(fy[...], mbuf[:, pl.ds(n * 4 * nz, 4 * nz)], preferred_element_type=f32)
            for i in range(4):
                ybuf[k, 4 * n + i] = out[:, i * nz : (i + 1) * nz].astype(bf16)

    def send_lines(k):
        for a, b, c in order:
            d = (lax.rem(col // 8 + a, 2) * 4 + lax.rem(col // 2 + b, 4)) * 2 + lax.rem(col + c, 2)
            pltpu.make_async_remote_copy(
                src_ref=ybuf.at[k, d],
                dst_ref=recv.at[k, col],
                send_sem=send_sem.at[k],
                recv_sem=recv_sem.at[k],
                device_id={"row": row, "col": d},
                device_id_type=MESH,
            ).start()
        recv[k, col] = ybuf[k, col]

    def halo_copy(src, dst, r, d, way):
        return pltpu.make_async_remote_copy(
            src_ref=src.at[d],
            dst_ref=dst.at[col],
            send_sem=hsend_sem.at[way],
            recv_sem=hrecv_sem.at[way],
            device_id={"row": r, "col": d},
            device_id_type=MESH,
        )

    field_loads[0].wait()
    filter_lines(0)

    @pl.when(col != GATE)
    def _():
        pl.semaphore_wait(barrier, ncol - 1)
        pl.semaphore_signal(joined, inc=1, device_id={"row": row, "col": GATE}, device_id_type=MESH)

    @pl.when(col == GATE)
    def _():
        pl.semaphore_wait(joined, ncol - 1)
        for r in (above, below):
            pl.semaphore_signal(barrier, inc=1, device_id={"row": r, "col": GATE}, device_id_type=MESH)

    send_lines(0)

    @pl.loop(1, EARLY)
    def _(k):
        pltpu.make_async_copy(field.at[:, k], fbuf.at[k], fsem.at[k]).wait()
        filter_lines(k)
        send_lines(k)

    for copy in edge_loads:
        copy.wait()
    for d in range(ncol):
        parts = []
        for l in range(lines):
            x = d * lines + l
            parts.append(etop[d, l].astype(f32) * mask_rows(0, x))
            parts.append(ebot[d, l].astype(f32) * mask_rows(nyb - 1, x))
        mbuf[:, pl.ds(d * nz, nz)] = jnp.concatenate(parts, axis=0).astype(bf16)
    for n in range(ncol // 4):
        halo = jnp.dot(ch[...], mbuf[:, pl.ds(n * 4 * nz, 4 * nz)], preferred_element_type=f32).astype(bf16)
        for i in range(4):
            hup[4 * n + i] = halo[: 3 * lines, i * nz : (i + 1) * nz]
            hdown[4 * n + i] = halo[3 * lines :, i * nz : (i + 1) * nz]

    @pl.when(col == GATE)
    def _():
        pl.semaphore_wait(barrier, 2)
        for s in range(1, ncol):
            pl.semaphore_signal(
                rows_in, inc=1, device_id={"row": row, "col": lax.rem(col + s, ncol)}, device_id_type=MESH
            )

    @pl.when(col != GATE)
    def _():
        pl.semaphore_wait(rows_in, 1)

    @pl.loop(0, ncol)
    def _(s):
        d = lax.rem(col + s, ncol)
        halo_copy(hup, hfrom_next, above, d, 0).start()
        halo_copy(hdown, hfrom_prev, below, d, 1).start()

    @pl.loop(EARLY, lines)
    def _(k):
        pltpu.make_async_copy(field.at[:, k], fbuf.at[k], fsem.at[k]).wait()
        filter_lines(k)
        send_lines(k)

    for copy in late:
        copy.wait()

    def z_filter(block, j):
        near = [block((2 * j + o) % ncol) for o in (-1, 0, 1, 2)]
        out = jnp.dot(jnp.concatenate(near, axis=1), bz[...], preferred_element_type=f32)
        return out.astype(bf16)

    def arrive(k):
        arrived = recv.at[k, pl.ds(0, ncol - 1)]
        pltpu.make_async_copy(arrived, arrived, recv_sem.at[k]).wait()

    inner = pl.ds(8, ny - 16)
    last = lines - 1

    @pl.loop(0, last)
    def _(k):
        arrive(k)
        for j in range(ncol // 2):
            filt[k, inner, pl.ds(2 * j * nz, 2 * nz)] = z_filter(lambda c: recv[k, c, inner, :], j)

        @pl.loop(0, ncol // 2)
        def _(n):
            at = pl.ds(pl.multiple_of(n * (2 * nz), 2 * nz), 2 * nz)
            der[k, inner, at] = jnp.dot(filt[k, inner, :], dv[:, at], preferred_element_type=f32).astype(bf16)

    for way, ref in ((0, hfrom_next), (1, hfrom_prev)):
        pltpu.make_async_copy(ref, ref, hrecv_sem.at[way]).wait()
    for n in range(ncol // 4):
        halo = [
            jnp.concatenate([hfrom_next[c].astype(f32), hfrom_prev[c].astype(f32)], axis=0).astype(bf16)
            for c in range(4 * n, 4 * n + 4)
        ]
        out = jnp.dot(sp[...], jnp.concatenate(halo, axis=1), preferred_element_type=f32)
        for i in range(4):
            spread[4 * n + i] = out[:, i * nz : (i + 1) * nz]
    for c in range(ncol):
        own = []
        for l in range(last):
            own.append(recv[l, c, pl.ds(0, 8), :].astype(f32))
            own.append(recv[l, c, pl.ds(ny - 8, 8), :].astype(f32))
        edges[c] = (jnp.concatenate(own, axis=0) + spread[c, pl.ds(0, 16 * last), :]).astype(bf16)
    for j in range(ncol // 2):
        at = pl.ds(2 * j * nz, 2 * nz)
        out = z_filter(lambda c: edges[c], j)
        tail[pl.ds(ny, 16 * last), at] = out
        for l in range(last):
            filt[l, pl.ds(0, 8), at] = out[16 * l : 16 * l + 8]
            filt[l, pl.ds(ny - 8, 8), at] = out[16 * l + 8 : 16 * l + 16]

    arrive(last)
    for c in range(ncol):
        for lo, at in ((0, 0), (ny - 8, 8)):
            rows = pl.ds(lo, 8)
            recv[last, c, rows, :] = (
                recv[last, c, rows, :].astype(f32) + spread[c, pl.ds(16 * last + at, 8), :]
            ).astype(bf16)
    for j in range(ncol // 2):
        at = pl.ds(2 * j * nz, 2 * nz)
        out = z_filter(lambda c: recv[last, c], j)
        tail[pl.ds(0, ny), at] = out
        filt[last, :, at] = out

    for k in range(lines):
        sent = ybuf.at[k, pl.ds(0, ncol - 1)]
        pltpu.make_async_copy(sent, sent, send_sem.at[k]).wait()
    for way, ref in ((0, hup), (1, hdown)):
        pltpu.make_async_copy(ref, ref, hsend_sem.at[way]).wait()


def finish_kernel(filt, der, tail, dv, filt_out, der_out, dtail, sem, tail_sem):
    lines, ny, full = filt.shape
    inner = pl.ds(8, ny - 16)
    done = pl.ds(0, lines - 1)
    copies = [
        pltpu.make_async_copy(filt, filt_out, sem.at[0]),
        pltpu.make_async_copy(der.at[done, inner, :], der_out.at[done, inner, :], sem.at[1]),
    ]
    for copy in copies:
        copy.start()
    parts = 2
    width = full // parts
    for h in range(parts):
        at = pl.ds(h * width, width)
        dtail[:, at] = jnp.dot(tail[...], dv[:, at], preferred_element_type=jnp.float32).astype(jnp.bfloat16)
        copies.append(
            pltpu.make_async_copy(
                dtail.at[pl.ds(0, ny), at], der_out.at[lines - 1, :, at], tail_sem.at[h, 2 * lines - 2]
            )
        )
        copies[-1].start()
        for l in range(lines - 1):
            for e, lo in enumerate((0, ny - 8)):
                copies.append(
                    pltpu.make_async_copy(
                        dtail.at[pl.ds(ny + 16 * l + 8 * e, 8), at],
                        der_out.at[l, pl.ds(lo, 8), at],
                        tail_sem.at[h, 2 * l + e],
                    )
                )
                copies[-1].start()
    for copy in copies:
        copy.wait()


def shards(nrow, ncol, field, solid_flags, deriv_matrix):
    nx, ny, nz = field.shape
    nyb, nzb = solid_flags.shape[1:]
    lines = nx // ncol
    full = nz * ncol
    bf16, f32 = jnp.bfloat16, jnp.float32
    along_x = [(1, b, c) for b in (2, 1, 3, 0) for c in (0, 1)]
    along_y = [(0, b, c) for b in (2, 1, 3) for c in (0, 1)] + [(0, 0, 1)]
    order = [step for pair in zip(along_x, along_y) for step in pair] + along_x[len(along_y) :]
    out = (lines, ny, full)
    any_spec = pl.BlockSpec(memory_space=pl.ANY)
    vmem = pl.BlockSpec(memory_space=pltpu.VMEM)
    consts = [
        jnp.asarray(y_matrix(ny), bf16),
        jnp.asarray(halo_matrix(lines), bf16),
        jnp.asarray(spread_matrix(lines), bf16),
        jnp.asarray(z_matrix(nz), bf16),
        jnp.asarray(expand_matrix(nyb, nzb), bf16),
    ]
    tail = ny + 16 * (lines - 1)
    held = pl.pallas_call(
        functools.partial(exchange_kernel, nrow, ncol, order),
        name="exchange",
        out_shape=[pltpu.VMEM(shape, bf16) for shape in (out, out, (tail, full), (full, full))],
        in_specs=[any_spec, any_spec, any_spec, any_spec, any_spec, any_spec, any_spec, any_spec],
        out_specs=[vmem] * 4,
        scratch_shapes=[
            pltpu.VMEM((lines, ncol, ny, nz), bf16),
            pltpu.VMEM((ncol, lines, 8, nz), bf16),
            pltpu.VMEM((ncol, lines, 8, nz), bf16),
            pltpu.VMEM((nyb, nx, nz), f32),
            pltpu.VMEM((ny, full), bf16),
            pltpu.VMEM((lines, ncol, ny, nz), bf16),
            pltpu.VMEM((lines, ncol, ny, nz), bf16),
            pltpu.VMEM((ncol, 3 * lines, nz), bf16),
            pltpu.VMEM((ncol, 3 * lines, nz), bf16),
            pltpu.VMEM((ncol, 3 * lines, nz), bf16),
            pltpu.VMEM((ncol, 3 * lines, nz), bf16),
            pltpu.VMEM((ncol, 16 * lines, nz), f32),
            pltpu.VMEM((ncol, 16 * (lines - 1), nz), bf16),
            *[pltpu.VMEM(c.shape, c.dtype) for c in consts],
            pltpu.VMEM((nyb * nzb, nx), jnp.int32),
            pltpu.SemaphoreType.DMA((9,)),
            pltpu.SemaphoreType.DMA((lines,)),
            pltpu.SemaphoreType.DMA((lines,)),
            pltpu.SemaphoreType.DMA((lines,)),
            pltpu.SemaphoreType.DMA((2,)),
            pltpu.SemaphoreType.DMA((2,)),
            pltpu.SemaphoreType.REGULAR,
            pltpu.SemaphoreType.REGULAR,
        ],
        compiler_params=pltpu.CompilerParams(
            collective_id=0, has_side_effects=True, vmem_limit_bytes=45 * 1024 * 1024
        ),
    )(
        field.reshape(ncol, lines, ny, nz),
        jnp.transpose(solid_flags, (1, 2, 0)).reshape(nyb * nzb, nx),
        deriv_matrix,
        *consts,
    )
    return pl.pallas_call(
        finish_kernel,
        name="finish",
        out_shape=[jax.ShapeDtypeStruct(out, bf16)] * 2,
        in_specs=[vmem] * 4,
        out_specs=[any_spec, any_spec],
        scratch_shapes=[
            pltpu.VMEM((tail, full), bf16),
            pltpu.SemaphoreType.DMA((2,)),
            pltpu.SemaphoreType.DMA((2, 2 * lines - 1)),
        ],
        compiler_params=pltpu.CompilerParams(vmem_limit_bytes=8 * 1024 * 1024),
    )(*held)


def solution(mesh):
    in_specs = (P(None, "row", "col"), P(None, "row", "col"), P())
    out_specs = (P("col", "row", None), P("col", "row", None))
    body = functools.partial(shards, mesh.shape["row"], mesh.shape["col"])
    return jax.shard_map(body, mesh=mesh, in_specs=in_specs, out_specs=out_specs, check_vma=False)
```

```python
import functools

import jax
import jax.numpy as jnp
import numpy as np
from jax import lax
from jax.experimental import pallas as pl
from jax.experimental.pallas import tpu as pltpu
from jax.sharding import PartitionSpec as P

MESH = pl.DeviceIdType.MESH
GATE = 15
EARLY = 5
YBLK = 8
ZBLK = 16
TAPS = {-3: 1.0, -2: -6.0, -1: 15.0, 0: 44.0, 1: 15.0, 2: -6.0, 3: 1.0}


def y_matrix(ny):
    out = np.zeros((ny, ny), np.float32)
    for r in range(ny):
        for o, tap in TAPS.items():
            if 0 <= r + o < ny:
                out[r, r + o] = tap / 64.0
    return out


def halo_matrix(lines):
    up = np.zeros((lines * 3, lines * 16), np.float32)
    down = np.zeros((lines * 3, lines * 16), np.float32)
    for l in range(lines):
        for j in range(3):
            for q in range(3):
                o = q - (j - 3)
                if o in TAPS:
                    up[l * 3 + j, l * 16 + q] = TAPS[o] / 64.0
                o = (q - 3) - j
                if o in TAPS:
                    down[l * 3 + j, l * 16 + 8 + 5 + q] = TAPS[o] / 64.0
    return np.concatenate([up, down], axis=0)


def spread_matrix(lines):
    out = np.zeros((lines * 16, lines * 6), np.float32)
    for l in range(lines):
        for j in range(3):
            out[l * 16 + 8 + 5 + j, l * 3 + j] = 1.0
            out[l * 16 + j, lines * 3 + l * 3 + j] = 1.0
    return out


def z_matrix(nz):
    out = np.zeros((4 * nz, 2 * nz), np.float32)
    for c in range(2 * nz):
        for o, tap in TAPS.items():
            out[nz + c + o, c] = tap / 64.0
    return out


def expand_matrix(nyb, nzb):
    return np.kron(np.eye(nyb, dtype=np.float32), np.repeat(np.eye(nzb, dtype=np.float32), ZBLK, axis=1))


def exchange_kernel(
    nrow, ncol, order,
    field, flags_in, dmat, fy_in, ch_in, sp_in, bz_in, ex_in,
    filt, der, tail, dv,
    fbuf, etop, ebot, mask, mbuf, ybuf, recv, hup, hdown, hfrom_next, hfrom_prev, spread, edges,
    fy, ch, sp, bz, ex, flags,
    in_sem, fsem, send_sem, recv_sem, hsend_sem, hrecv_sem, joined, rows_in,
):
    row, col = lax.axis_index("row"), lax.axis_index("col")
    above, below = lax.rem(row + nrow - 1, nrow), lax.rem(row + 1, nrow)
    lines, ny, nz = fbuf.shape[0], fbuf.shape[2], fbuf.shape[3]
    nyb = ny // YBLK
    bf16, f32 = jnp.bfloat16, jnp.float32

    flag_loads = [
        pltpu.make_async_copy(flags_in, flags, in_sem.at[7]),
        pltpu.make_async_copy(ex_in, ex, in_sem.at[8]),
        pltpu.make_async_copy(fy_in, fy, in_sem.at[3]),
    ]
    field_loads = [pltpu.make_async_copy(field.at[:, k], fbuf.at[k], fsem.at[k]) for k in range(lines)]
    edge_loads = [
        pltpu.make_async_copy(field.at[:, :, pl.ds(0, 8), :], etop, in_sem.at[0]),
        pltpu.make_async_copy(field.at[:, :, pl.ds(ny - 8, 8), :], ebot, in_sem.at[1]),
        pltpu.make_async_copy(ch_in, ch, in_sem.at[2]),
    ]
    late = [
        pltpu.make_async_copy(sp_in, sp, in_sem.at[4]),
        pltpu.make_async_copy(bz_in, bz, in_sem.at[5]),
        pltpu.make_async_copy(dmat, dv, in_sem.at[6]),
    ]
    for copy in [*flag_loads, field_loads[0], *edge_loads, *field_loads[1:], *late]:
        copy.start()

    barrier = pltpu.get_barrier_semaphore()
    for s in range(1, ncol):
        d = lax.rem(col + s, ncol)

        @pl.when(d != GATE)
        def _():
            pl.semaphore_signal(barrier, inc=1, device_id={"row": row, "col": d}, device_id_type=MESH)

    for copy in flag_loads:
        copy.wait()
    per_line = flags[...].astype(f32).T.astype(bf16)
    for n in range(nyb // 4):
        solid = jnp.dot(per_line, ex[:, pl.ds(n * 4 * nz, 4 * nz)], preferred_element_type=f32)
        for b in range(4):
            mask[4 * n + b] = 1.0 - solid[:, b * nz : (b + 1) * nz]

    def mask_rows(b, x):
        return jnp.broadcast_to(mask[b, pl.ds(x, 1), :], (YBLK, nz))

    def filter_lines(k):
        for d in range(ncol):
            x = d * lines + k
            keep = jnp.concatenate([mask_rows(b, x) for b in range(nyb)], axis=0)
            mbuf[:, pl.ds(d * nz, nz)] = (fbuf[k, d].astype(f32) * keep).astype(bf16)
        for n in range(ncol // 4):
            out = jnp.dot(fy[...], mbuf[:, pl.ds(n * 4 * nz, 4 * nz)], preferred_element_type=f32)
            for i in range(4):
                ybuf[k, 4 * n + i] = out[:, i * nz : (i + 1) * nz].astype(bf16)

    def send_lines(k):
        for a, b, c in order:
            d = (lax.rem(col // 8 + a, 2) * 4 + lax.rem(col // 2 + b, 4)) * 2 + lax.rem(col + c, 2)
            pltpu.make_async_remote_copy(
                src_ref=ybuf.at[k, d],
                dst_ref=recv.at[k, col],
                send_sem=send_sem.at[k],
                recv_sem=recv_sem.at[k],
                device_id={"row": row, "col": d},
                device_id_type=MESH,
            ).start()
        recv[k, col] = ybuf[k, col]

    def halo_copy(src, dst, r, d, way):
        return pltpu.make_async_remote_copy(
            src_ref=src.at[d],
            dst_ref=dst.at[col],
            send_sem=hsend_sem.at[way],
            recv_sem=hrecv_sem.at[way],
            device_id={"row": r, "col": d},
            device_id_type=MESH,
        )

    field_loads[0].wait()
    filter_lines(0)

    @pl.when(col != GATE)
    def _():
        pl.semaphore_wait(barrier, ncol - 1)
        pl.semaphore_signal(joined, inc=1, device_id={"row": row, "col": GATE}, device_id_type=MESH)

    @pl.when(col == GATE)
    def _():
        pl.semaphore_wait(joined, ncol - 1)
        for r in (above, below):
            pl.semaphore_signal(barrier, inc=1, device_id={"row": r, "col": GATE}, device_id_type=MESH)

    send_lines(0)

    @pl.loop(1, EARLY)
    def _(k):
        pltpu.make_async_copy(field.at[:, k], fbuf.at[k], fsem.at[k]).wait()
        filter_lines(k)
        send_lines(k)

    for copy in edge_loads:
        copy.wait()
    for d in range(ncol):
        parts = []
        for l in range(lines):
            x = d * lines + l
            parts.append(etop[d, l].astype(f32) * mask_rows(0, x))
            parts.append(ebot[d, l].astype(f32) * mask_rows(nyb - 1, x))
        mbuf[:, pl.ds(d * nz, nz)] = jnp.concatenate(parts, axis=0).astype(bf16)
    for n in range(ncol // 4):
        halo = jnp.dot(ch[...], mbuf[:, pl.ds(n * 4 * nz, 4 * nz)], preferred_element_type=f32).astype(bf16)
        for i in range(4):
            hup[4 * n + i] = halo[: 3 * lines, i * nz : (i + 1) * nz]
            hdown[4 * n + i] = halo[3 * lines :, i * nz : (i + 1) * nz]

    @pl.when(col == GATE)
    def _():
        pl.semaphore_wait(barrier, 2)
        for s in range(1, ncol):
            pl.semaphore_signal(
                rows_in, inc=1, device_id={"row": row, "col": lax.rem(col + s, ncol)}, device_id_type=MESH
            )

    @pl.when(col != GATE)
    def _():
        pl.semaphore_wait(rows_in, 1)

    @pl.loop(0, ncol)
    def _(s):
        d = lax.rem(col + s, ncol)
        halo_copy(hup, hfrom_next, above, d, 0).start()
        halo_copy(hdown, hfrom_prev, below, d, 1).start()

    @pl.loop(EARLY, lines)
    def _(k):
        pltpu.make_async_copy(field.at[:, k], fbuf.at[k], fsem.at[k]).wait()
        filter_lines(k)
        send_lines(k)

    for copy in late:
        copy.wait()

    def z_filter(block, j):
        near = [block((2 * j + o) % ncol) for o in (-1, 0, 1, 2)]
        out = jnp.dot(jnp.concatenate(near, axis=1), bz[...], preferred_element_type=f32)
        return out.astype(bf16)

    def arrive(k):
        arrived = recv.at[k, pl.ds(0, ncol - 1)]
        pltpu.make_async_copy(arrived, arrived, recv_sem.at[k]).wait()

    inner = pl.ds(8, ny - 16)
    last = lines - 1

    @pl.loop(0, last)
    def _(k):
        arrive(k)
        for j in range(ncol // 2):
            filt[k, inner, pl.ds(2 * j * nz, 2 * nz)] = z_filter(lambda c: recv[k, c, inner, :], j)

        @pl.loop(0, ncol // 2)
        def _(n):
            at = pl.ds(pl.multiple_of(n * (2 * nz), 2 * nz), 2 * nz)
            der[k, inner, at] = jnp.dot(filt[k, inner, :], dv[:, at], preferred_element_type=f32).astype(bf16)

    for way, ref in ((0, hfrom_next), (1, hfrom_prev)):
        pltpu.make_async_copy(ref, ref, hrecv_sem.at[way]).wait()
    for n in range(ncol // 4):
        halo = [
            jnp.concatenate([hfrom_next[c].astype(f32), hfrom_prev[c].astype(f32)], axis=0).astype(bf16)
            for c in range(4 * n, 4 * n + 4)
        ]
        out = jnp.dot(sp[...], jnp.concatenate(halo, axis=1), preferred_element_type=f32)
        for i in range(4):
            spread[4 * n + i] = out[:, i * nz : (i + 1) * nz]
    for c in range(ncol):
        own = []
        for l in range(last):
            own.append(recv[l, c, pl.ds(0, 8), :].astype(f32))
            own.append(recv[l, c, pl.ds(ny - 8, 8), :].astype(f32))
        edges[c] = (jnp.concatenate(own, axis=0) + spread[c, pl.ds(0, 16 * last), :]).astype(bf16)
    for j in range(ncol // 2):
        at = pl.ds(2 * j * nz, 2 * nz)
        out = z_filter(lambda c: edges[c], j)
        tail[pl.ds(ny, 16 * last), at] = out
        for l in range(last):
            filt[l, pl.ds(0, 8), at] = out[16 * l : 16 * l + 8]
            filt[l, pl.ds(ny - 8, 8), at] = out[16 * l + 8 : 16 * l + 16]

    arrive(last)
    for c in range(ncol):
        for lo, at in ((0, 0), (ny - 8, 8)):
            rows = pl.ds(lo, 8)
            recv[last, c, rows, :] = (
                recv[last, c, rows, :].astype(f32) + spread[c, pl.ds(16 * last + at, 8), :]
            ).astype(bf16)
    for j in range(ncol // 2):
        at = pl.ds(2 * j * nz, 2 * nz)
        out = z_filter(lambda c: recv[last, c], j)
        tail[pl.ds(0, ny), at] = out
        filt[last, :, at] = out

    for k in range(lines):
        sent = ybuf.at[k, pl.ds(0, ncol - 1)]
        pltpu.make_async_copy(sent, sent, send_sem.at[k]).wait()
    for way, ref in ((0, hup), (1, hdown)):
        pltpu.make_async_copy(ref, ref, hsend_sem.at[way]).wait()


def finish_kernel(filt, der, tail, dv, filt_out, der_out, dtail, sem, tail_sem):
    lines, ny, full = filt.shape
    inner = pl.ds(8, ny - 16)
    done = pl.ds(0, lines - 1)
    copies = [
        pltpu.make_async_copy(filt, filt_out, sem.at[0]),
        pltpu.make_async_copy(der.at[done, inner, :], der_out.at[done, inner, :], sem.at[1]),
    ]
    for copy in copies:
        copy.start()
    parts = 2
    width = full // parts
    for h in range(parts):
        at = pl.ds(h * width, width)
        dtail[:, at] = jnp.dot(tail[...], dv[:, at], preferred_element_type=jnp.float32).astype(jnp.bfloat16)
        copies.append(
            pltpu.make_async_copy(
                dtail.at[pl.ds(0, ny), at], der_out.at[lines - 1, :, at], tail_sem.at[h, 2 * lines - 2]
            )
        )
        copies[-1].start()
        for l in range(lines - 1):
            for e, lo in enumerate((0, ny - 8)):
                copies.append(
                    pltpu.make_async_copy(
                        dtail.at[pl.ds(ny + 16 * l + 8 * e, 8), at],
                        der_out.at[l, pl.ds(lo, 8), at],
                        tail_sem.at[h, 2 * l + e],
                    )
                )
                copies[-1].start()
    for copy in copies:
        copy.wait()


def shards(nrow, ncol, field, solid_flags, deriv_matrix):
    nx, ny, nz = field.shape
    nyb, nzb = solid_flags.shape[1:]
    lines = nx // ncol
    full = nz * ncol
    bf16, f32 = jnp.bfloat16, jnp.float32
    along_x = [(1, b, c) for b in (2, 1, 3, 0) for c in (0, 1)]
    along_y = [(0, b, c) for b in (2, 1, 3) for c in (0, 1)] + [(0, 0, 1)]
    order = [step for pair in zip(along_x, along_y) for step in pair] + along_x[len(along_y) :]
    out = (lines, ny, full)
    any_spec = pl.BlockSpec(memory_space=pl.ANY)
    vmem = pl.BlockSpec(memory_space=pltpu.VMEM)
    consts = [
        jnp.asarray(y_matrix(ny), bf16),
        jnp.asarray(halo_matrix(lines), bf16),
        jnp.asarray(spread_matrix(lines), bf16),
        jnp.asarray(z_matrix(nz), bf16),
        jnp.asarray(expand_matrix(nyb, nzb), bf16),
    ]
    tail = ny + 16 * (lines - 1)
    held = pl.pallas_call(
        functools.partial(exchange_kernel, nrow, ncol, order),
        name="exchange",
        out_shape=[pltpu.VMEM(shape, bf16) for shape in (out, out, (tail, full), (full, full))],
        in_specs=[any_spec, any_spec, any_spec, any_spec, any_spec, any_spec, any_spec, any_spec],
        out_specs=[vmem] * 4,
        scratch_shapes=[
            pltpu.VMEM((lines, ncol, ny, nz), bf16),
            pltpu.VMEM((ncol, lines, 8, nz), bf16),
            pltpu.VMEM((ncol, lines, 8, nz), bf16),
            pltpu.VMEM((nyb, nx, nz), f32),
            pltpu.VMEM((ny, full), bf16),
            pltpu.VMEM((lines, ncol, ny, nz), bf16),
            pltpu.VMEM((lines, ncol, ny, nz), bf16),
            pltpu.VMEM((ncol, 3 * lines, nz), bf16),
            pltpu.VMEM((ncol, 3 * lines, nz), bf16),
            pltpu.VMEM((ncol, 3 * lines, nz), bf16),
            pltpu.VMEM((ncol, 3 * lines, nz), bf16),
            pltpu.VMEM((ncol, 16 * lines, nz), f32),
            pltpu.VMEM((ncol, 16 * (lines - 1), nz), bf16),
            *[pltpu.VMEM(c.shape, c.dtype) for c in consts],
            pltpu.VMEM((nyb * nzb, nx), jnp.int32),
            pltpu.SemaphoreType.DMA((9,)),
            pltpu.SemaphoreType.DMA((lines,)),
            pltpu.SemaphoreType.DMA((lines,)),
            pltpu.SemaphoreType.DMA((lines,)),
            pltpu.SemaphoreType.DMA((2,)),
            pltpu.SemaphoreType.DMA((2,)),
            pltpu.SemaphoreType.REGULAR,
            pltpu.SemaphoreType.REGULAR,
        ],
        compiler_params=pltpu.CompilerParams(
            collective_id=0, has_side_effects=True, vmem_limit_bytes=45 * 1024 * 1024
        ),
    )(
        field.reshape(ncol, lines, ny, nz),
        jnp.transpose(solid_flags, (1, 2, 0)).reshape(nyb * nzb, nx),
        deriv_matrix,
        *consts,
    )
    return pl.pallas_call(
        finish_kernel,
        name="finish",
        out_shape=[jax.ShapeDtypeStruct(out, bf16)] * 2,
        in_specs=[vmem] * 4,
        out_specs=[any_spec, any_spec],
        scratch_shapes=[
            pltpu.VMEM((tail, full), bf16),
            pltpu.SemaphoreType.DMA((2,)),
            pltpu.SemaphoreType.DMA((2, 2 * lines - 1)),
        ],
        compiler_params=pltpu.CompilerParams(vmem_limit_bytes=8 * 1024 * 1024),
    )(*held)


def solution(mesh):
    in_specs = (P(None, "row", "col"), P(None, "row", "col"), P())
    out_specs = (P("col", "row", None), P("col", "row", None))
    body = functools.partial(shards, mesh.shape["row"], mesh.shape["col"])
    return jax.shard_map(body, mesh=mesh, in_specs=in_specs, out_specs=out_specs, check_vma=False)
```
